16 devices in a mesh: dp: 4 (over y, z, core), tp: 4 (over x).
Axes of the slice: x: 4, y: 2, z: 1, core: 2. Of those that a mesh axis runs over, the one named last changes fastest.
The devices are a block of a 4x4x8 slice.
Arguments:
- x: bfloat16 [4096, 6144], P(('dp', 'tp')), parts along dimension 0
- dy: bfloat16 [4096, 6144], P(('dp', 'tp')), parts along dimension 0
- gain: bfloat16 [6144], replicated
- wq: bfloat16 [6144, 6144], P(None, 'tp')
- wk: bfloat16 [6144, 512], P(None, 'tp')
- wv: bfloat16 [6144, 512], P(None, 'tp')
- wo: bfloat16 [6144, 6144], P('tp')
Outputs:
- output 1: bfloat16 [4096, 6144], P(('dp', 'tp')), parts along dimension 0
- output 2: float32 [4, 6144], P('dp'), parts along dimension 0
- output 3: bfloat16 [24576, 6144], P('dp', 'tp'), parts along dimension 0
- output 4: bfloat16 [24576, 512], P('dp', 'tp'), parts along dimension 0
- output 5: bfloat16 [24576, 512], P('dp', 'tp'), parts along dimension 0
- output 6: bfloat16 [24576, 6144], P(('dp', 'tp')), parts along dimension 0
There are 4 independent parts. The reference program is written for one: setup_inputs(seed, part) draws one part's arguments, and reference() takes and returns one part's arrays. A program takes and returns all parts, laid end to end along the dimension named above; an argument that names none is the same for every part.
All inputs are finite; a program needn't handle non-finite values.
Results may differ from the reference program's by a relative error of at most 0.018.
Values are sent between devices in bfloat16 or wider.
A program may use at most 768 MiB of HBM per device.

```python
import jax
import jax.numpy as jnp
from jax import lax

ROWS = 1024
D = 6144
HEADS = 48
KV_HEADS = 4
HEAD = 128
THETA = 10000


def setup_inputs(seed: int = 0, part: int = 0) -> dict:
    kx, ky, kn, kq, kk, kv, ko = jax.random.split(jax.random.key(seed), 7)

    def weights(key, rows, columns):
        return jax.random.normal(key, (rows, columns), jnp.float32) * rows**-0.5

    drawn = {
        "x": jax.random.normal(jax.random.fold_in(kx, part), (ROWS, D), jnp.float32),
        "dy": jax.random.normal(jax.random.fold_in(ky, part), (ROWS, D), jnp.float32) * ROWS**-0.5,
        "gain": 1 + 0.1 * jax.random.normal(kn, (D,), jnp.float32),
        "wq": 2 * weights(kq, D, HEADS * HEAD),
        "wk": 2 * weights(kk, D, KV_HEADS * HEAD),
        "wv": 4 * weights(kv, D, KV_HEADS * HEAD),
        "wo": weights(ko, HEADS * HEAD, D),
    }
    return {k: v.astype(jnp.bfloat16) for k, v in drawn.items()}


def normed(x, gain):
    wide = x.astype(jnp.float32)
    scale = lax.rsqrt(jnp.mean(wide * wide, -1, keepdims=True) + 1e-6)
    return (wide * scale * gain.astype(jnp.float32)).astype(jnp.bfloat16)


def turned(t, place, theta):
    half = t.shape[-1] // 2
    angle = place.astype(jnp.float32)[:, None] * theta ** (-jnp.arange(half, dtype=jnp.float32) / half)
    cos, sin = jnp.cos(angle)[:, None], jnp.sin(angle)[:, None]
    a, b = t[..., :half].astype(jnp.float32), t[..., half:].astype(jnp.float32)
    return jnp.concatenate([a * cos - b * sin, b * cos + a * sin], -1).astype(jnp.bfloat16)


def matmul(a, w):
    return jnp.dot(a, w, preferred_element_type=jnp.float32).astype(jnp.bfloat16)


def einsum(form, a, b):
    return jnp.einsum(form, a.astype(jnp.float32), b.astype(jnp.float32))


def attention(q, k, v):
    scores = einsum("tgsd,ugd->gstu", q, k) * q.shape[-1] ** -0.5
    token = jnp.arange(q.shape[0])
    scores = jnp.where(token[:, None] >= token, scores, -jnp.inf)
    weights = jax.nn.softmax(scores, -1).astype(jnp.bfloat16)
    return einsum("gstu,ugd->tgsd", weights, v).astype(jnp.bfloat16)


def forward(x, gain, wq, wk, wv, wo):
    rows = x.shape[0]
    a, place = normed(x, gain), jnp.arange(rows)
    k = turned(matmul(a, wk).reshape(rows, -1, HEAD), place, THETA)
    q = turned(matmul(a, wq).reshape(rows, -1, HEAD), place, THETA).reshape(rows, k.shape[1], -1, HEAD)
    v = matmul(a, wv).reshape(rows, -1, HEAD)
    seen = attention(q, k, v).reshape(rows, -1)
    return (x.astype(jnp.float32) + jnp.dot(seen, wo, preferred_element_type=jnp.float32)).astype(jnp.bfloat16)


def reference(x, dy, gain, wq, wk, wv, wo):
    _, back = jax.vjp(forward, x, gain.astype(jnp.float32), wq, wk, wv, wo)
    by_x, by_gain, *by_weights = back(dy)
    return (by_x, by_gain[None], *by_weights)
```

```python
import functools

import jax
import jax.numpy as jnp
from jax import lax
from jax.experimental import pallas as pl
from jax.experimental.pallas import tpu as pltpu
from jax.sharding import PartitionSpec as P


NEG = -1e30
HIDDEN = 2 * NEG
LOG2E = 1.4426950408889634
VMEM = 56 * 2**20
HEAD = 128
THETA = 10000
PAIR = 2


def _dot(a, b, ca, cb):
    return lax.dot_general(a, b, (((ca,), (cb,)), ((), ())), preferred_element_type=jnp.float32)


def _slot(distance):
    return jnp.where(distance == 2, 3, jnp.where(distance == 3, 2, distance))


def _strip(ref, h):
    return jnp.concatenate([ref[:, i * HEAD : (i + 1) * HEAD] for i in range(h, h + PAIR)], axis=0)


def _lower(keys, queries):
    shape = (keys, PAIR * queries)
    return lax.rem(lax.broadcasted_iota(jnp.int32, shape, 1), queries) >= lax.broadcasted_iota(jnp.int32, shape, 0)


def _forward(me_ref, q_ref, cos_ref, sin_ref, k_ref, v_ref, o_ref, turned_ref, lse_ref, top_s, mix_s, *, n, heads, scale):
    bq = q_ref.shape[0]
    slot, me = pl.program_id(0), me_ref[0]
    place = lax.rem(me + _slot(slot), n)
    e = scale * LOG2E
    cos, sin = cos_ref[...], sin_ref[...]
    for h in range(heads):
        t = q_ref[:, h * HEAD : (h + 1) * HEAD].astype(jnp.float32)
        turned_ref[:, h * HEAD : (h + 1) * HEAD] = (t * cos + pltpu.roll(t, HEAD // 2, 1) * sin).astype(jnp.bfloat16)
    top_s[...] = jnp.full_like(top_s, NEG)
    mix_s[...] = jnp.zeros_like(mix_s)
    ones = jnp.ones((8, bq), jnp.bfloat16)

    def block(at, masked):
        here = pl.ds(pl.multiple_of(at * bq, bq), bq)
        keys = k_ref[here, :]
        values = jnp.concatenate([v_ref[here, :].T, ones], axis=0)
        scores = [_dot(keys, _strip(turned_ref, h), 1, 1) for h in range(0, heads, PAIR)]
        ok = _lower(bq, bq) if masked else None
        weights, keeps = [], []
        for i, s in enumerate(scores):
            if masked:
                s = jnp.where(ok, s, HIDDEN)
            old = top_s[i : i + 1, :]
            top = jnp.maximum(old, s.max(axis=0, keepdims=True))
            top_s[i : i + 1, :] = top
            weights.append(jnp.exp2((s - top) * e).astype(jnp.bfloat16))
            keeps.append(jnp.exp2((old - top) * e))
        for i, (p, keep) in enumerate(zip(weights, keeps)):
            mix_s[i] = mix_s[i] * keep + _dot(values, p, 1, 0)

    lax.fori_loop(0, place, lambda j, _: block(_slot(lax.rem(j - me + n, n)), False), None)
    block(slot, True)
    for i in range(heads // PAIR):
        top, total = top_s[i : i + 1, :], mix_s[i, HEAD : HEAD + 1, :]
        out = (mix_s[i, :HEAD, :] * (1 / total)).T.astype(o_ref.dtype)
        lse = top * scale + jnp.log(total)
        for m in range(PAIR):
            h = i * PAIR + m
            o_ref[:, h * HEAD : (h + 1) * HEAD] = out[m * bq : (m + 1) * bq, :]
            lse_ref[0, h : h + 1, :] = lse[:, m * bq : (m + 1) * bq]


def attend(me, qkv, k, v, cos, sin, n):
    rows, bq = k.shape[0], k.shape[0] // n
    width = qkv.shape[1] - 2 * HEAD
    heads = width // HEAD
    block = lambda w: pl.BlockSpec((bq, w), lambda i, _: (i, 0))
    whole = pl.BlockSpec((rows, HEAD), lambda i, _: (0, 0))
    pairs = heads // PAIR
    return pl.pallas_call(
        functools.partial(_forward, n=n, heads=heads, scale=HEAD**-0.5),
        grid_spec=pltpu.PrefetchScalarGridSpec(
            num_scalar_prefetch=1,
            grid=(n,),
            in_specs=[block(width), block(HEAD), block(HEAD), whole, whole],
            out_specs=[block(width), block(width), pl.BlockSpec((1, heads, bq), lambda i, _: (i, 0, 0))],
            scratch_shapes=[pltpu.VMEM((pairs, PAIR * bq), jnp.float32), pltpu.VMEM((pairs, HEAD + 8, PAIR * bq), jnp.float32)],
        ),
        out_shape=[
            jax.ShapeDtypeStruct((rows, width), jnp.bfloat16),
            jax.ShapeDtypeStruct((rows, width), jnp.bfloat16),
            jax.ShapeDtypeStruct((n, heads, bq), jnp.float32),
        ],
        compiler_params=pltpu.CompilerParams(dimension_semantics=("arbitrary",), vmem_limit_bytes=VMEM),
        cost_estimate=pl.CostEstimate(flops=20_000_000_000, transcendentals=heads * rows * rows // 2, bytes_accessed=6 * rows * width),
        name="attend",
    )(me, qkv, cos, sin, k, v)


def _backward(me_ref, q_ref, o_ref, lse_ref, do_ref, cos_ref, sin_ref, k_ref, v_ref, dk0_ref, dv0_ref, dq_ref, dk_ref, dv_ref, dq_s,
              *, n, first, heads, scale):
    bq = q_ref.shape[0]
    step, me = pl.program_id(0), me_ref[0]
    slot = step + first
    place = lax.rem(me + _slot(slot), n)
    e = scale * LOG2E

    @pl.when(step == 0)
    def _():
        dk_ref[...] = dk0_ref[...]
        dv_ref[...] = dv0_ref[...]

    dq_s[...] = jnp.zeros_like(dq_s)
    starts = range(0, heads, PAIR)
    lses = [jnp.concatenate([lse_ref[0, h + m : h + m + 1, :] for m in range(PAIR)], axis=1) * LOG2E for h in starts]
    deltas = [(_strip(do_ref, h).astype(jnp.float32) * _strip(o_ref, h).astype(jnp.float32)).T.sum(axis=0, keepdims=True) for h in starts]

    def block(at, masked):
        here = pl.ds(pl.multiple_of(at * bq, bq), bq)
        keys, values = k_ref[here, :], v_ref[here, :]
        qs = [_strip(q_ref, h) for h in starts]
        dos = [_strip(do_ref, h) for h in starts]
        scores = [_dot(keys, x, 1, 1) for x in qs]
        dps = [_dot(values, x, 1, 1) for x in dos]
        ok = _lower(bq, bq) if masked else None
        across = keys.T
        for i in range(len(qs)):
            p = jnp.exp2(scores[i] * e - lses[i])
            if masked:
                p = jnp.where(ok, p, 0.0)
            ds = (p * (dps[i] - deltas[i])).astype(jnp.bfloat16)
            dv_ref[here, :] += _dot(p.astype(jnp.bfloat16), dos[i], 1, 0)
            dk_ref[here, :] += _dot(ds, qs[i], 1, 0)
            dq_s[i] += _dot(across, ds, 1, 0)

    lax.fori_loop(0, place, lambda j, _: block(_slot(lax.rem(j - me + n, n)), False), None)
    block(slot, True)
    cos, sin = cos_ref[...], sin_ref[...]
    for i in range(heads // PAIR):
        dq = (dq_s[i] * scale).T
        for m in range(PAIR):
            h, t = i * PAIR + m, dq[m * bq : (m + 1) * bq, :]
            dq_ref[:, h * HEAD : (h + 1) * HEAD] = (t * cos - pltpu.roll(t, HEAD // 2, 1) * sin).astype(dq_ref.dtype)


def attend_bwd(me, q, o, lse, d_out, cos, sin, k, v, dk, dv, first, n):
    rows, bq = k.shape[0], k.shape[0] // n
    width = d_out.shape[1]
    heads = width // HEAD
    steps = d_out.shape[0] // bq
    block = lambda w: pl.BlockSpec((bq, w), lambda i, _: (i + first, 0))
    own = pl.BlockSpec((bq, width), lambda i, _: (i, 0))
    whole = pl.BlockSpec((rows, HEAD), lambda i, _: (0, 0))
    return pl.pallas_call(
        functools.partial(_backward, n=n, first=first, heads=heads, scale=HEAD**-0.5),
        grid_spec=pltpu.PrefetchScalarGridSpec(
            num_scalar_prefetch=1,
            grid=(steps,),
            in_specs=[block(width), block(width), pl.BlockSpec((1, heads, bq), lambda i, _: (i + first, 0, 0)), own, block(HEAD), block(HEAD),
                      whole, whole, whole, whole],
            out_specs=[own, whole, whole],
            scratch_shapes=[pltpu.VMEM((heads // PAIR, HEAD, PAIR * bq), jnp.float32)],
        ),
        out_shape=[
            jax.ShapeDtypeStruct((steps * bq, width), jnp.bfloat16),
            jax.ShapeDtypeStruct((rows, HEAD), jnp.float32),
            jax.ShapeDtypeStruct((rows, HEAD), jnp.float32),
        ],
        compiler_params=pltpu.CompilerParams(dimension_semantics=("arbitrary",), vmem_limit_bytes=VMEM),
        cost_estimate=pl.CostEstimate(flops=7_000_000_000 * steps, transcendentals=heads * rows * rows // 8 * steps,
                                      bytes_accessed=8 * steps * bq * width),
        name="attend_bwd",
    )(me, q, o, lse, d_out, cos, sin, k, v, dk, dv)


def scale_of(wide):
    return lax.rsqrt(jnp.mean(wide * wide, -1, keepdims=True) + 1e-6)


def normed(x, gain):
    wide = x.astype(jnp.float32)
    return (wide * scale_of(wide) * gain).astype(jnp.bfloat16)


def tables(me, rows, n):
    half = HEAD // 2
    row = lax.iota(jnp.int32, rows)
    bq = rows // n
    place = lax.rem(me + _slot(row // bq), n) * bq + row % bq
    angle = place.astype(jnp.float32)[:, None] * THETA ** (-jnp.arange(half, dtype=jnp.float32) / half)
    cos, sin = jnp.cos(angle), jnp.sin(angle)
    return jnp.concatenate([cos, cos], 1), jnp.concatenate([-sin, sin], 1)


def solution(mesh):
    n = mesh.shape["tp"]
    to_right = [(i, (i + 1) % n) for i in range(n)]
    to_left = [(i, (i - 1) % n) for i in range(n)]

    def right(t):
        return lax.ppermute(t, "tp", to_right)

    def left(t):
        return lax.ppermute(t, "tp", to_left)

    bf16, f32 = jnp.bfloat16, jnp.float32

    def spread(upper, lower):
        la, rb = right(upper), left(lower)
        lb, ra = right(lower), left(upper)
        oa, ob = right(la), left(rb)
        return jnp.concatenate([ra, rb, la, lb]), jnp.concatenate([oa, ob])

    def work(x, dy, gain, wq, wk, wv, wo):
        me = lax.axis_index("tp")
        bq, depth = x.shape
        h = bq // 2
        rows = n * bq
        g = gain.astype(f32)
        cos, sin = tables(me, rows, n)
        who = me[None].astype(jnp.int32)
        wide = wq.shape[1]

        upper, lower = normed(x[:h], g), normed(x[h:], g)
        sides, opposite = spread(upper, lower)
        own = jnp.concatenate([upper, lower])
        w = jnp.concatenate([wq, wk, wv], axis=1)

        def project(a):
            return _dot(a, w, 1, 0).astype(bf16)

        qkv = jnp.concatenate([project(own), project(sides), project(opposite)])
        k, v = qkv[:, wide : wide + HEAD], qkv[:, wide + HEAD :]
        kf = k.astype(f32)
        k = (kf * cos + jnp.roll(kf, HEAD // 2, 1) * sin).astype(bf16)
        seen, q, lse = attend(who, qkv, k, v, cos, sin, n)

        dy_sides, dy_opposite = spread(dy[:h], dy[h:])

        def into(t):
            return _dot(t, wo, 1, 1).astype(bf16)

        zero = jnp.zeros((rows, HEAD), f32)
        dq0, dk, dv = attend_bwd(who, q, seen, lse, into(dy), cos, sin, k, v, zero, zero, 0, n)
        dq1, dk, dv = attend_bwd(who, q, seen, lse, into(dy_sides), cos, sin, k, v, dk, dv, 1, n)
        dq2, dk, dv = attend_bwd(who, q, seen, lse, into(dy_opposite), cos, sin, k, v, dk, dv, 3, n)
        dk = dk * HEAD**-0.5
        dk = (dk * cos - jnp.roll(dk, HEAD // 2, 1) * sin).astype(bf16)
        dkv = jnp.concatenate([dk, dv.astype(bf16)], axis=1)

        def terms(dq, dkv, more=None):
            t = _dot(jnp.concatenate([dq, dkv], axis=1), w, 1, 1)
            return t if more is None else t + more.astype(f32)

        far = terms(dq2, dkv[3 * bq :]).astype(bf16)
        ra, lb = right(far[:h]), left(far[h:])
        near = terms(dq1[h : h + bq], dkv[bq + h : 2 * bq + h]).astype(bf16)
        fb, ga = right(near[:h]), left(near[h:])
        ends = lambda t, a: jnp.concatenate([t[a : a + h], t[a + bq + h : a + 2 * bq]])
        last = terms(ends(dq1, 0), ends(dkv, bq), jnp.concatenate([ra, lb])).astype(bf16)
        fa, gb = right(last[:h]), left(last[h:])
        mine = lax.optimization_barrier(terms(dq0, dkv[:bq]))

        a_all = jnp.concatenate([own, sides, opposite])
        dy_all = jnp.concatenate([dy, dy_sides, dy_opposite])
        dq = jnp.concatenate([dq0, dq1, dq2])
        by_wo = _dot(seen, dy_all, 0, 0).astype(bf16)
        by_wq = _dot(a_all, dq, 0, 0).astype(bf16)
        by_kv = _dot(a_all, dkv, 0, 0).astype(bf16)

        wx = x.astype(f32)
        scale = scale_of(wx)
        got = jnp.concatenate([fa.astype(f32) + ga.astype(f32), fb.astype(f32) + gb.astype(f32)])
        d_a = mine + got
        part = (d_a * wx * scale).sum(0, keepdims=True)
        d_n = d_a * g
        by_x = dy.astype(f32) + scale * d_n - wx * (scale**3 / depth) * (d_n * wx).sum(-1, keepdims=True)
        across = lax.ppermute(part, "tp", [(i, (i + 2) % n) for i in range(n)])
        by_gain = (part + across) + (right(part) + left(part))
        return by_x.astype(bf16), by_gain, by_wq, by_kv[:, :HEAD], by_kv[:, HEAD:], by_wo

    tokens, columns = P(("dp", "tp"), None), P(None, "tp")
    return jax.shard_map(
        work,
        mesh=mesh,
        in_specs=(tokens, tokens, P(None), columns, columns, columns, P("tp", None)),
        out_specs=(tokens, P("dp", None), P("dp", "tp"), P("dp", "tp"), P("dp", "tp"), P(("dp", "tp"), None)),
        check_vma=False,
    )
```
